128 devices in a mesh: don: 8 (over x, core), acc: 16 (over y, z).
Axes of the slice: x: 4, y: 4, z: 4, core: 2. Of those that a mesh axis runs over, the one named last changes fastest.
Arguments:
- donor_emb: bfloat16 [262144, 768], P(('don', 'acc')), may hold values from -12 to 12
- acceptor_emb: bfloat16 [262144, 768], P(('don', 'acc')), may hold values from -6 to 6
- donor_pos: int32 [3072], P(('don', 'acc')), may hold values from 0 to 2047
- acceptor_pos: int32 [3072], P(('don', 'acc')), may hold values from 0 to 2047
- donor_count: int32 [128], P('don'), may hold values from 1 to 24, as said below
- acceptor_count: int32 [128], replicated, may hold values from 1 to 24, as said below
- target: int32 [64, 3072], P(None, 'don'), may hold values from 0 to 3071, as said below
- junction_mask: int32 [64, 3072], P(None, 'don'), may hold values 0 or 1
- weights: bfloat16 [64, 768, 768], P('acc'), may hold values from -1 to 2
Outputs:
- loss: float32 [], replicated
- grad_weight: float32 [768, 64, 768], P('don', 'acc')
The draws below stay inside these ranges and needn't reach their ends.
Inputs may be any that keep to these rules, and one draw needn't show every extreme that they name: `donor_count`: the live donor slots of all shards number exactly 1600; some shard has all 24 live. `acceptor_count`: the live acceptor slots of all shards number exactly 1600; some shard has all 24 live. `target`: each entry names a live acceptor slot.
All inputs are finite; a program needn't handle non-finite values. No bound on the sum of `junction_mask` on one device may be relied on, other than what follows from the above.
Results may differ from the reference program's by a relative error of at most 0.0031.
Values may be sent and summed in bfloat16 or wider, within the bound.
No kernel may reach another device: no remote copies, remote signals or barrier semaphores. Data moves between devices by JAX's collectives and lax.ppermute only.
A program may use at most 128 MiB of HBM per device.

```python
import jax
import jax.numpy as jnp
from jax import lax

D = 768
TIS = 64
CAP = 24
POS_DEV = 2048
SHARDS = 128
SEQ = 262144
DONORS = 3072


def site_counts(key):
    bias_key, noise_key, chosen_key = jax.random.split(key, 3)
    extra = CAP - 1
    slots = SHARDS * extra
    needed = SHARDS * (CAP + 1) // 2 - SHARDS
    bias = jax.random.randint(bias_key, (SHARDS,), 0, 8)
    chosen = jax.random.randint(chosen_key, (), 0, SHARDS)
    bias = jnp.where(jnp.arange(SHARDS) == chosen, 12, bias)
    noise = jax.random.randint(noise_key, (SHARDS, extra), 0, 65536)
    score = noise + bias[:, None] * 16384
    order = jnp.arange(slots, dtype=jnp.int32).reshape(SHARDS, extra)
    keyed = (score * slots + order).reshape(-1).astype(jnp.int32)
    threshold = jnp.sort(keyed)[slots - needed]
    taken = (keyed >= threshold).astype(jnp.int32).reshape(SHARDS, extra)
    return (1 + jnp.sum(taken, axis=1)).astype(jnp.int32)


def draw_donor_count(key, part):
    return site_counts(jax.random.fold_in(key, 3))


def draw_acceptor_count(key, part):
    return site_counts(jax.random.fold_in(key, 5))


def draw_target(key, part):
    counts = site_counts(jax.random.fold_in(key, 5))
    shard_key, slot_key = jax.random.split(jax.random.fold_in(key, 11))
    shard = jax.random.randint(shard_key, (TIS, DONORS), 0, SHARDS)
    within = jax.random.randint(slot_key, (TIS, DONORS), 0, counts[shard])
    return (shard * CAP + within).astype(jnp.int32)


def draw_donor_emb(key, part):
    noise_key = jax.random.fold_in(jax.random.fold_in(key, 21), 0)
    values = jax.random.truncated_normal(noise_key, -6.0, 6.0, (SEQ, D), jnp.float32)
    return values.astype(jnp.bfloat16)


def draw_acceptor_emb(key, part):
    noise_key = jax.random.fold_in(key, 23)
    values = jax.random.truncated_normal(noise_key, -6.0, 6.0, (SEQ, D), jnp.float32)
    return values.astype(jnp.bfloat16)


def draw_weights(key, part):
    values = jax.random.truncated_normal(jax.random.fold_in(key, 31), -4.0, 4.0, (TIS, D, D), jnp.float32) * D ** (-0.5)
    return values.astype(jnp.bfloat16)


def touch_ends(drawn, stream_key, low, high):
    extent = drawn.shape
    spot = [jax.random.randint(jax.random.fold_in(stream_key, axis), (), 0, extent[axis]) for axis in range(len(extent))]
    drawn = drawn.at[tuple(spot)].set(low)
    longest = extent.index(max(extent))
    spot[longest] = (spot[longest] + 1) % extent[longest]
    return drawn.at[tuple(spot)].set(high)


def setup_inputs(seed: int = 0) -> dict:
    key_list = jax.random.split(jax.random.key(seed), 10)
    return {
        "donor_emb": draw_donor_emb(jax.random.fold_in(key_list[9], 71), 0),
        "acceptor_emb": draw_acceptor_emb(jax.random.fold_in(key_list[9], 71), 0),
        "donor_pos": touch_ends(jax.random.randint(key_list[2], (DONORS,), 0, POS_DEV), jax.random.fold_in(key_list[2], 1), 0, POS_DEV - 1).astype(jnp.int32),
        "acceptor_pos": touch_ends(jax.random.randint(key_list[3], (DONORS,), 0, POS_DEV), jax.random.fold_in(key_list[3], 1), 0, POS_DEV - 1).astype(jnp.int32),
        "donor_count": draw_donor_count(jax.random.fold_in(key_list[9], 71), 0),
        "acceptor_count": draw_acceptor_count(jax.random.fold_in(key_list[9], 71), 0),
        "target": draw_target(jax.random.fold_in(key_list[9], 71), 0),
        "junction_mask": touch_ends((jax.random.randint(key_list[7], (TIS, DONORS), 0, 2) < 1).astype(jnp.int32), jax.random.fold_in(key_list[7], 1), 0, 1),
        "weights": draw_weights(jax.random.fold_in(key_list[9], 71), 0),
    }


def site_rows(emb, positions):
    slot = jnp.arange(positions.shape[0], dtype=jnp.int32)
    rows = ((slot // CAP) * POS_DEV + positions).astype(jnp.int32)
    return jnp.take(emb, rows, axis=0)


def live_slots(counts):
    slot = jnp.arange(DONORS, dtype=jnp.int32)
    return (slot % CAP) < jnp.repeat(counts, CAP)


def reference(donor_emb, acceptor_emb, donor_pos, acceptor_pos, donor_count, acceptor_count, target, junction_mask, weights):
    donors = site_rows(donor_emb, donor_pos)
    acceptors = site_rows(acceptor_emb, acceptor_pos)
    live_d = live_slots(donor_count)
    live_a = live_slots(acceptor_count)
    scale = D ** -0.5
    columns = jnp.arange(DONORS, dtype=jnp.int32)

    def tissue(inputs):
        matrix, target_row, mask_row = inputs
        projected = jnp.dot(donors, matrix, preferred_element_type=jnp.float32).astype(jnp.bfloat16)
        scores = jnp.dot(projected, acceptors.T, preferred_element_type=jnp.float32) * scale
        scores = jnp.where(live_a[None, :], scores, -1e30)
        highest = jnp.max(scores, axis=1, keepdims=True)
        summed_exp = jnp.sum(jnp.where(live_a[None, :], jnp.exp(scores - highest), 0.0), axis=1, keepdims=True)
        log_total = highest + jnp.log(summed_exp)
        is_target = columns[None, :] == target_row[:, None]
        picked = jnp.sum(jnp.where(is_target, scores, 0.0), axis=1)
        weight = jnp.where(live_d, mask_row, 0).astype(jnp.float32)
        summed = jnp.sum(weight * (log_total[:, 0] - picked))
        counted = jnp.sum(weight)
        probs = jnp.where(live_a[None, :], jnp.exp(scores - log_total), 0.0)
        dscore = (weight[:, None] * (probs - is_target.astype(jnp.float32))).astype(jnp.bfloat16)
        dproj = (jnp.dot(dscore, acceptors, preferred_element_type=jnp.float32) * scale).astype(jnp.bfloat16)
        gradient = jnp.dot(donors.T, dproj, preferred_element_type=jnp.float32)
        return summed, counted, gradient

    summed, counted, gradient = lax.map(tissue, (weights, target, junction_mask))
    loss = jnp.sum(summed) / jnp.maximum(jnp.sum(counted), 1.0)
    return loss, jnp.transpose(gradient, (1, 0, 2))
```

```python
import itertools

import jax
import jax.numpy as jnp
from jax import lax
from jax.experimental import pallas as pl
from jax.experimental.pallas import tpu as pltpu
from jax.sharding import Mesh
from jax.sharding import PartitionSpec as P


AXES = ("x", "c", "y", "z")
SIZES = (4, 2, 4, 4)
CAP = 24
LIVE = 1600
COLS = 1664
ROWS_A = 1744
MB = 256
PIECE = 16 * CAP
SUB = 128
F32 = jnp.float32
BF16 = jnp.bfloat16
I32 = jnp.int32


def exchange_pairs(axis_core0, axis_core1, mask):
    pairs = []
    for coords in itertools.product(*(range(n) for n in SIZES)):
        moved = list(coords)
        axis = AXES.index(axis_core1 if coords[1] else axis_core0)
        moved[axis] ^= mask
        source = target = 0
        for n, a, b in zip(SIZES, coords, moved):
            source, target = source * n + a, target * n + b
        pairs.append((source, target))
    return pairs


def exchange(value, axis_core0, axis_core1, mask):
    return lax.ppermute(value, AXES, exchange_pairs(axis_core0, axis_core1, mask))


def swap_core(value):
    return lax.ppermute(value, "c", [(0, 1), (1, 0)])


def compact(dst_ref, source, rank_row, start):
    base = pl.multiple_of((start // 16) * 16, 16)
    hit = lax.broadcasted_iota(I32, (SUB + 16, SUB), 0) == rank_row - base
    picked = jnp.dot(
        jnp.where(hit, 1.0, 0.0).astype(BF16), source, preferred_element_type=F32
    ).astype(BF16)
    dst_ref[pl.ds(base, 16), :] = dst_ref[pl.ds(base, 16), :] + picked[:16]
    dst_ref[pl.ds(base + 16, SUB), :] = picked[16:]
    return hit, base


def acceptor_kernel(starts_ref, rank_ref, *refs):
    pieces, out_ref = refs[:-1], refs[-1]
    out_ref[0:16, :] = jnp.zeros((16, out_ref.shape[1]), BF16)
    blocks = PIECE // SUB
    for i, piece in enumerate(pieces):
        for j in range(blocks):
            b = i * blocks + j
            compact(out_ref, piece[j * SUB : (j + 1) * SUB, :], rank_ref[b : b + 1, :], starts_ref[b])
    out_ref[LIVE:COLS, :] = jnp.zeros((COLS - LIVE, out_ref.shape[1]), BF16)


def head_kernel(starts_ref, coord_ref, off_ref, val_ref, acc_ref, w_ref, *refs):
    pieces = refs[:-7]
    keep_ref, send_ref, sums_ref, rows_ref, tval_ref, grad_ref, num_ref = refs[-7:]
    width = w_ref.shape[0]
    scale = width ** (-0.5)
    x, c, y, z = (coord_ref[i] for i in range(4))
    blocks = PIECE // SUB
    count = starts_ref[len(pieces) * blocks]

    val = val_ref[...]
    active = jnp.where(val >= 0, 1.0, 0.0)
    lower = lax.broadcasted_iota(I32, (SUB, SUB), 0) <= lax.broadcasted_iota(I32, (SUB, SUB), 1)
    inclusive = jnp.dot(
        active.astype(BF16), jnp.where(lower, 1.0, 0.0).astype(BF16), preferred_element_type=F32
    ).astype(I32)

    rows_ref[0:16, :] = jnp.zeros((16, width), BF16)
    tval_ref[0:16, :] = jnp.zeros((16, SUB), I32)
    for i, piece in enumerate(pieces):
        for j in range(blocks):
            b = i * blocks + j
            start = starts_ref[b]
            row = val[b : b + 1, :]
            rank = jnp.where(row >= 0, inclusive[b : b + 1, :] - 1 + start, -1)
            hit, base = compact(rows_ref, piece[j * SUB : (j + 1) * SUB, :], rank, start)
            chosen = jnp.sum(jnp.where(hit, row, 0), axis=1, keepdims=True)
            chosen = jnp.broadcast_to(chosen, (SUB + 16, SUB))
            tval_ref[pl.ds(base, 16), :] = tval_ref[pl.ds(base, 16), :] + chosen[:16]
            tval_ref[pl.ds(base + 16, SUB), :] = chosen[16:]
    tail = pl.multiple_of(((count + 15) // 16) * 16, 16)
    rows_ref[pl.ds(tail, MB), :] = jnp.zeros((MB, width), BF16)
    tval_ref[pl.ds(tail, MB), :] = jnp.zeros((MB, SUB), I32)

    grad_ref[...] = jnp.zeros((width, width), F32)
    num_ref[...] = jnp.zeros((8, SUB), F32)

    def block(i, carry):
        first = pl.multiple_of(i * MB, MB)
        donors = rows_ref[pl.ds(first, MB), :]
        slot = tval_ref[pl.ds(first, MB), :]
        shard = (slot * 2731) >> 16
        within = slot - shard * CAP
        mx = (shard >> 5) ^ x
        core = (shard >> 4) & 1
        my = ((shard >> 2) & 3) ^ y
        mz = (shard & 3) ^ z
        place = jnp.where(core == 0, mx * 16 + mz * 4 + my, my * 16 + mx * 4 + mz)
        place = place + jnp.where(core == c, 0, 64)
        found = place == lax.broadcasted_iota(I32, (MB, SUB), 1)
        column = jnp.sum(jnp.where(found, off_ref[0:1, :] + within, 0), axis=1, keepdims=True)

        projected = jnp.dot(donors, w_ref[...], preferred_element_type=F32).astype(BF16)
        acceptors = acc_ref[0:COLS, :]
        scores = (
            lax.dot_general(
                projected, acceptors, (((1,), (1,)), ((), ())), preferred_element_type=F32
            )
            * scale
        )
        columns = lax.broadcasted_iota(I32, (MB, COLS), 1)
        scores = jnp.where(columns < LIVE, scores, -1e30)
        highest = jnp.max(scores, axis=1, keepdims=True)
        exped = jnp.where(columns < LIVE, jnp.exp(scores - highest), 0.0)
        summed = jnp.sum(exped, axis=1, keepdims=True)
        is_target = columns == column
        picked = jnp.sum(jnp.where(is_target, scores, 0.0), axis=1, keepdims=True)
        here = first + lax.broadcasted_iota(I32, (MB, 1), 0) < count
        loss = jnp.where(here, highest + jnp.log(summed) - picked, 0.0)
        num_ref[0:1, :] = num_ref[0:1, :] + jnp.sum(loss)
        probs = exped * (1.0 / summed)
        dscore = jnp.where(here, probs - jnp.where(is_target, 1.0, 0.0), 0.0).astype(BF16)
        dproj = (jnp.dot(dscore, acceptors, preferred_element_type=F32) * scale).astype(BF16)
        grad_ref[...] += lax.dot_general(
            donors, dproj, (((0,), (0,)), ((), ())), preferred_element_type=F32
        )
        return carry

    lax.fori_loop(0, (count + MB - 1) // MB, block, 0)

    lanes = lax.broadcasted_iota(I32, (8, SUB), 1)
    sums_ref[...] = jnp.where(lanes == 0, num_ref[0:1, :], count.astype(F32))
    part = width // 8
    for i in range(4):
        keep_ref[i] = grad_ref[pl.ds(pl.multiple_of((2 * i + c) * part, 8), part), :]
        send_ref[i] = grad_ref[pl.ds(pl.multiple_of((2 * i + 1 - c) * part, 8), part), :]


def local(
    donor_emb,
    acceptor_emb,
    donor_pos,
    acceptor_pos,
    donor_count,
    acceptor_count,
    target,
    junction_mask,
    weights,
):
    width = weights.shape[1]
    x, c, y, z = (lax.axis_index(a) for a in AXES)
    vmem = pl.BlockSpec(memory_space=pltpu.VMEM)
    smem = pl.BlockSpec(memory_space=pltpu.SMEM)

    acceptor_local = jnp.take(acceptor_emb, acceptor_pos, axis=0)
    donor_local = jnp.take(donor_emb, donor_pos, axis=0)

    first = 4 * (y * 4 + z)
    targets = lax.dynamic_slice_in_dim(target, first, 4, 0)
    masks = lax.dynamic_slice_in_dim(junction_mask, first, 4, 0)
    live = jnp.arange(PIECE, dtype=I32) % CAP < jnp.repeat(donor_count, CAP)
    value = jnp.where(live[None, :] & (masks > 0), targets, -1).reshape(4, 3, SUB)
    received = [lax.dynamic_index_in_dim(value, x, 0, False)]
    for m in (1, 2, 3):
        received.append(exchange(lax.dynamic_index_in_dim(value, x ^ m, 0, False), "x", "x", m))

    block = jnp.concatenate([acceptor_local, donor_local])
    block = jnp.stack([block] + [exchange(block, "y", "z", m) for m in (1, 2, 3)])
    block = jnp.stack([block] + [exchange(block, "z", "x", m) for m in (1, 2, 3)])
    acceptors = block[:, :, :CAP].reshape(PIECE, width)
    donors = block[:, :, CAP:].reshape(PIECE, width)
    acceptors = [acceptors] + [exchange(acceptors, "x", "y", m) for m in (1, 2, 3)]
    donors = [donors] + [exchange(donors, "x", "y", m) for m in (1, 2, 3)]
    others = [swap_core(piece) for piece in acceptors]

    places = jnp.arange(128, dtype=I32)
    m3, m2, m1 = (places >> 4) & 3, (places >> 2) & 3, places & 3
    core = c ^ (places >> 6)
    shard0 = ((x ^ m3) * 2) * 16 + (y ^ m1) * 4 + (z ^ m2)
    shard1 = ((x ^ m2) * 2 + 1) * 16 + (y ^ m3) * 4 + (z ^ m1)
    shard = jnp.where(core == 0, shard0, shard1)
    counts = jnp.sum(
        jnp.where(shard[:, None] == places[None, :], acceptor_count[None, :], 0), axis=1
    )
    offsets = jnp.sum(jnp.where(places[None, :] < places[:, None], counts[None, :], 0), axis=1)
    within = jnp.arange(CAP, dtype=I32)
    rank = jnp.where(within[None, :] < counts[:, None], offsets[:, None] + within[None, :], -1)
    rank = rank.reshape(24, SUB)
    edges = jnp.arange(25, dtype=I32) * SUB
    starts_a = jnp.sum(
        jnp.clip(edges[:, None] - CAP * places[None, :], 0, counts[None, :]), axis=1
    )

    natural = jnp.stack(received).reshape(64, CAP).astype(F32)
    place = jnp.arange(64, dtype=I32)
    m3, m2, m1 = (place >> 4) & 3, (place >> 2) & 3, place & 3
    natural_index = jnp.where(
        c == 0,
        m3 * 16 + (y ^ m1) * 4 + (z ^ m2),
        m2 * 16 + (y ^ m3) * 4 + (z ^ m1),
    )
    onehot = (natural_index[:, None] == place[None, :]).astype(F32)
    ordered = jnp.dot(onehot, natural, precision=lax.Precision.HIGHEST)
    ordered = jnp.round(ordered).astype(I32).reshape(12, SUB)
    per_block = jnp.sum((ordered >= 0).astype(I32), axis=1)
    twelve = jnp.arange(13, dtype=I32)
    starts_d = jnp.sum(
        jnp.where(twelve[None, :12] < twelve[:, None], per_block[None, :], 0), axis=1
    )

    compacted = pl.pallas_call(
        acceptor_kernel,
        out_shape=jax.ShapeDtypeStruct((ROWS_A, width), BF16),
        in_specs=[smem] + [vmem] * 9,
        out_specs=vmem,
        name="acceptor_compact",
    )(starts_a, rank, *acceptors, *others)

    tissue = lax.dynamic_index_in_dim(weights, x, 0, False)
    coords = jnp.stack([x, c, y, z]).astype(I32)
    part = width // 8
    keep, send, sums = pl.pallas_call(
        head_kernel,
        out_shape=(
            jax.ShapeDtypeStruct((4, part, width), F32),
            jax.ShapeDtypeStruct((4, part, width), F32),
            jax.ShapeDtypeStruct((8, SUB), F32),
        ),
        in_specs=[smem, smem] + [vmem] * 8,
        out_specs=(vmem, vmem, vmem),
        scratch_shapes=[
            pltpu.VMEM((4 * PIECE + MB + 16, width), BF16),
            pltpu.VMEM((4 * PIECE + MB + 16, SUB), I32),
            pltpu.VMEM((width, width), F32),
            pltpu.VMEM((8, SUB), F32),
        ],
        name="junction_head",
    )(starts_d, coords, offsets.reshape(1, 128), ordered, compacted, tissue, *donors)

    total = (keep + swap_core(send)).astype(BF16)
    spread = lax.all_to_all(total, "x", 0, 0, tiled=True)
    grad_weight = jnp.transpose(spread, (1, 0, 2)).astype(F32)

    sums = sums + swap_core(sums)
    sums = jnp.broadcast_to(sums[None], (64, 8, SUB))
    sums = lax.all_to_all(sums, ("x", "y", "z"), 0, 0, tiled=True)
    sums = jnp.sum(sums[:, 0, :2], axis=0)
    loss = sums[0] / jnp.maximum(sums[1], 1.0)
    return (loss, grad_weight)


def solution(mesh):
    finer = Mesh(mesh.devices.reshape(SIZES), AXES)
    don, acc = ("x", "c"), ("y", "z")
    return jax.shard_map(
        local,
        mesh=finer,
        in_specs=(
            P(AXES, None),
            P(AXES, None),
            P(AXES),
            P(AXES),
            P(don),
            P(),
            P(None, don),
            P(None, don),
            P(acc, None, None),
        ),
        out_specs=(P(), P(don, acc, None)),
        check_vma=False,
    )
```

```python
import itertools

import jax
import jax.numpy as jnp
from jax import lax
from jax.experimental import pallas as pl
from jax.experimental.pallas import tpu as pltpu
from jax.sharding import Mesh
from jax.sharding import PartitionSpec as P


AXES = ("x", "c", "y", "z")
SIZES = (4, 2, 4, 4)
CAP = 24
LIVE = 1600
COLS = 1664
ROWS_A = 1744
MAIN = 1536
MB = 256
PIECE = 16 * CAP
SUB = 128
F32 = jnp.float32
BF16 = jnp.bfloat16
I32 = jnp.int32


def exchange_pairs(axis_core0, axis_core1, mask):
    pairs = []
    for coords in itertools.product(*(range(n) for n in SIZES)):
        moved = list(coords)
        axis = AXES.index(axis_core1 if coords[1] else axis_core0)
        moved[axis] ^= mask
        source = target = 0
        for n, a, b in zip(SIZES, coords, moved):
            source, target = source * n + a, target * n + b
        pairs.append((source, target))
    return pairs


def exchange(value, axis_core0, axis_core1, mask):
    return lax.ppermute(value, AXES, exchange_pairs(axis_core0, axis_core1, mask))


def swap_core(value):
    return lax.ppermute(value, "c", [(0, 1), (1, 0)])


def site_kernel(
    apos_ref,
    dpos_ref,
    count_ref,
    aemb_ref,
    demb_ref,
    target_ref,
    mask_ref,
    out_ref,
    rows_ref,
    picked_ref,
    sems,
):
    sites = 2 * CAP
    copies = []
    picks = lax.broadcasted_iota(I32, (sites, 8 * sites), 0)
    lanes = lax.broadcasted_iota(I32, (sites, 8 * sites), 1)
    column = lax.axis_index("y") * 4 + lax.axis_index("z")
    tissues = pl.multiple_of((column // 2) * 8, 8)
    for i, ref in enumerate((target_ref, mask_ref)):
        copies.append(
            pltpu.make_async_copy(
                ref.at[pl.ds(tissues, 8), :], picked_ref.at[i], sems.at[sites + i]
            )
        )
        copies[-1].start()
    wanted = picks * 8
    for i in range(sites):
        emb_ref, pos = (aemb_ref, apos_ref[i]) if i < CAP else (demb_ref, dpos_ref[i - CAP])
        group = pl.multiple_of((pos // 8) * 8, 8)
        copies.append(
            pltpu.make_async_copy(
                emb_ref.at[pl.ds(group, 8), :], rows_ref.at[pl.ds(8 * i, 8), :], sems.at[i]
            )
        )
        copies[-1].start()
        wanted = jnp.where(picks == i, wanted + (pos - group), wanted)
    onehot = jnp.where(lanes == wanted, 1.0, 0.0).astype(BF16)

    lane = lax.broadcasted_iota(I32, (4, PIECE), 1)
    shard = (lane * 2731) >> 16
    limit = jnp.zeros((4, PIECE), I32)
    for i in range(16):
        limit = jnp.where(shard == i, count_ref[i], limit)
    live = lane - shard * CAP < limit
    for copy in copies[:2]:
        copy.wait()
    upper = column % 2 == 1
    targets = jnp.where(upper, picked_ref[0, 4:8, :], picked_ref[0, 0:4, :])
    masks = jnp.where(upper, picked_ref[1, 4:8, :], picked_ref[1, 0:4, :])
    value = jnp.where(live & (masks > 0), targets, -1)
    halves = jnp.concatenate([value >> 6, value & 63], axis=1).astype(F32)
    halves = jnp.concatenate([halves, jnp.zeros_like(halves)], axis=0)
    out_ref[sites : sites + 8, :] = halves.astype(BF16)

    for copy in copies[2:]:
        copy.wait()
    out_ref[0:sites, :] = jnp.dot(
        onehot, rows_ref[...], preferred_element_type=F32
    ).astype(BF16)


def output_kernel(own_ref, one_ref, two_ref, three_ref, out_ref):
    x = lax.axis_index("x")
    for m, ref in enumerate((own_ref, one_ref, two_ref, three_ref)):
        out_ref[:, pl.ds(x ^ m, 1), :] = ref[...].astype(F32)[:, None, :]


def one_hot(hit):
    return jnp.where(hit, 1.0, 0.0).astype(BF16)


def as_rows(row):
    return jnp.broadcast_to(row, (8, SUB)).astype(BF16)


def acceptor_tables(count_row, x, c, y, z):
    lane = lax.broadcasted_iota(I32, (1, SUB), 1)
    sub = lax.broadcasted_iota(I32, (SUB, SUB), 0)
    m3, m2, m1 = (lane >> 4) & 3, (lane >> 2) & 3, lane & 3
    core = c ^ (lane >> 6)
    shard0 = (x ^ m3) * 32 + (y ^ m1) * 4 + (z ^ m2)
    shard1 = (x ^ m2) * 32 + 16 + (y ^ m3) * 4 + (z ^ m1)
    shard = jnp.where(core == 0, shard0, shard1)
    counts = jnp.dot(
        as_rows(count_row.astype(F32)), one_hot(sub == shard), preferred_element_type=F32
    )
    offsets = jnp.dot(
        counts.astype(BF16), one_hot(sub < lane), preferred_element_type=F32
    ).astype(I32)
    counts_row = counts.astype(I32)[0:1, :]
    row = lax.broadcasted_iota(I32, (8, SUB), 0)
    table = jnp.where(row == 0, counts.astype(I32), jnp.where(row == 1, offsets >> 6, offsets & 63))
    table = table.astype(F32).astype(BF16)
    ranks, starts = [], []
    for b in range(8 * PIECE // SUB):
        slot = b * SUB + lane
        place = (slot * 2731) >> 16
        within = slot - place * CAP
        here = jnp.dot(table, one_hot(sub == place), preferred_element_type=F32).astype(I32)
        rank = here[1:2, :] * 64 + here[2:3, :] + within
        ranks.append(jnp.where(within < here[0:1, :], rank, -1))
        before = jnp.minimum(jnp.maximum(b * SUB - CAP * lane, 0), counts_row)
        starts.append(jnp.sum(before.astype(F32)).astype(I32))
    return offsets[0:1, :], ranks, starts


def donor_tables(rows, x, c, y, z):
    lane = lax.broadcasted_iota(I32, (1, SUB), 1)
    sub = lax.broadcasted_iota(I32, (SUB, SUB), 0)
    row = lax.broadcasted_iota(I32, (8, SUB), 0)
    pick = lax.broadcasted_iota(I32, (8, 2 * PIECE), 0) == x
    lines = [
        jnp.sum(jnp.where(pick, r.astype(F32), 0.0), axis=0, keepdims=True) for r in rows
    ]
    sources = []
    for u in range(PIECE // SUB):
        low, high = u * SUB, (u + 1) * SUB
        stack = [line[:, low:high] for line in lines]
        stack += [line[:, PIECE + low : PIECE + high] for line in lines]
        sources.append(jnp.concatenate(stack, axis=0).astype(BF16))
    values = []
    for m3 in range(4):
        for v in range(PIECE // SUB):
            slot = v * SUB + lane
            place = (slot * 2731) >> 16
            within = slot - place * CAP
            m2, m1 = place >> 2, place & 3
            natural0 = (y ^ m1) * 4 + (z ^ m2)
            natural1 = (y ^ m3) * 4 + (z ^ m1)
            natural = jnp.where(c == 0, natural0, natural1) * CAP + within
            wanted = jnp.where(c == 0, m3, m2)
            moved = sum(
                jnp.dot(source, one_hot(sub + u * SUB == natural), preferred_element_type=F32)
                for u, source in enumerate(sources)
            )
            moved = jnp.where((row & 3) == wanted, moved, 0.0)
            moved = moved * jnp.where(row < 4, 64.0, 1.0)
            values.append(jnp.sum(moved, axis=0, keepdims=True).astype(I32))
    return values


def compact(dst_ref, source, rank_row, start):
    base = pl.multiple_of((start // 16) * 16, 16)
    hit = lax.broadcasted_iota(I32, (SUB + 16, SUB), 0) == rank_row - base
    picked = jnp.dot(
        jnp.where(hit, 1.0, 0.0).astype(BF16), source, preferred_element_type=F32
    ).astype(BF16)
    dst_ref[pl.ds(base, 16), :] = dst_ref[pl.ds(base, 16), :] + picked[:16]
    dst_ref[pl.ds(base + 16, SUB), :] = picked[16:]
    return hit, base


def acceptor_kernel(count_ref, lines_ref, *refs):
    pieces = refs[:8]
    acc_ref, offset_ref, value_ref, rank_ref, starts_ref = refs[8:]
    width = acc_ref.shape[1]
    x, c, y, z = (lax.axis_index(a) for a in AXES)
    blocks = PIECE // SUB

    rows = [
        jnp.where(c == 0, pieces[i][PIECE : PIECE + 8, :], lines_ref[i]) for i in range(4)
    ]
    lower = lax.broadcasted_iota(I32, (SUB, SUB), 0) <= lax.broadcasted_iota(I32, (SUB, SUB), 1)
    lower = one_hot(lower)
    count = 0
    for b, row in enumerate(donor_tables(rows, x, c, y, z)):
        starts_ref[b] = count
        active = jnp.where(row >= 0, 1.0, 0.0)
        inclusive = jnp.dot(as_rows(active), lower, preferred_element_type=F32).astype(I32)
        rank_ref[b : b + 1, :] = jnp.where(row >= 0, inclusive[0:1, :] - 1 + count, -1)
        value_ref[b : b + 1, :] = row
        count = count + jnp.sum(active).astype(I32)
    starts_ref[4 * blocks] = count

    offset_row, ranks, starts_a = acceptor_tables(count_ref[...], x, c, y, z)
    offset_ref[...] = jnp.broadcast_to(offset_row, (8, SUB))
    acc_ref[0:16, :] = jnp.zeros((16, width), BF16)
    for b in range(8 * blocks):
        i, j = b // blocks, b % blocks
        compact(acc_ref, pieces[i][j * SUB : (j + 1) * SUB, :], ranks[b], starts_a[b])
    acc_ref[LIVE:COLS, :] = jnp.zeros((COLS - LIVE, width), BF16)


def head_kernel(starts_ref, acc_ref, offset_ref, value_ref, rank_ref, w_ref, *refs):
    pieces = refs[:4]
    keep_ref, send_ref, sums_ref = refs[4:7]
    rows_ref, tval_ref, grad_ref, num_ref = refs[7:]
    width = w_ref.shape[0]
    scale = width ** (-0.5)
    x, c, y, z = (lax.axis_index(a) for a in AXES)
    blocks = PIECE // SUB
    count = starts_ref[4 * blocks]
    offset_row = offset_ref[0:1, :]

    rows_ref[0:16, :] = jnp.zeros((16, width), BF16)
    tval_ref[0:16, :] = jnp.zeros((16, SUB), I32)
    grad_ref[...] = jnp.zeros((width, width), F32)
    num_ref[...] = jnp.zeros((8, SUB), F32)
    for b in range(4 * blocks):
        i, j = b // blocks, b % blocks
        source = pieces[i][j * SUB : (j + 1) * SUB, :]
        hit, base = compact(rows_ref, source, rank_ref[b : b + 1, :], starts_ref[b])
        chosen = jnp.sum(jnp.where(hit, value_ref[b : b + 1, :], 0), axis=1, keepdims=True)
        chosen = jnp.broadcast_to(chosen, (SUB + 16, SUB))
        tval_ref[pl.ds(base, 16), :] = tval_ref[pl.ds(base, 16), :] + chosen[:16]
        tval_ref[pl.ds(base + 16, SUB), :] = chosen[16:]
    tail = pl.multiple_of(((count + 15) // 16) * 16, 16)
    rows_ref[pl.ds(tail, MB), :] = jnp.zeros((MB, width), BF16)
    tval_ref[pl.ds(tail, MB), :] = jnp.zeros((MB, SUB), I32)

    def block(i, carry):
        first = pl.multiple_of(i * MB, MB)
        donors = rows_ref[pl.ds(first, MB), :]
        slot = tval_ref[pl.ds(first, MB), :]
        shard = (slot * 2731) >> 16
        within = slot - shard * CAP
        mx = (shard >> 5) ^ x
        core = (shard >> 4) & 1
        my = ((shard >> 2) & 3) ^ y
        mz = (shard & 3) ^ z
        place = jnp.where(core == 0, mx * 16 + mz * 4 + my, my * 16 + mx * 4 + mz)
        place = place + jnp.where(core == c, 0, 64)
        found = place == lax.broadcasted_iota(I32, (MB, SUB), 1)
        column = jnp.sum(jnp.where(found, offset_row + within, 0), axis=1, keepdims=True)

        projected = jnp.dot(donors, w_ref[...], preferred_element_type=F32).astype(BF16)
        groups = ((0, MAIN), (MAIN, COLS))
        scores, targets = [], []
        for low, high in groups:
            part = lax.dot_general(
                projected,
                acc_ref[low:high, :],
                (((1,), (1,)), ((), ())),
                preferred_element_type=F32,
            )
            columns = low + lax.broadcasted_iota(I32, (MB, high - low), 1)
            part = part * scale
            if high > LIVE:
                part = jnp.where(columns < LIVE, part, -1e30)
            scores.append(part)
            targets.append(columns == column)
        highest = jnp.maximum(*(jnp.max(part, axis=1, keepdims=True) for part in scores))
        exped = [jnp.exp(part - highest) for part in scores]
        exped[1] = jnp.where(scores[1] > -1e29, exped[1], 0.0)
        summed = sum(jnp.sum(part, axis=1, keepdims=True) for part in exped)
        picked = sum(
            jnp.sum(jnp.where(hit, part, 0.0), axis=1, keepdims=True)
            for hit, part in zip(targets, scores)
        )
        here = first + lax.broadcasted_iota(I32, (MB, 1), 0) < count
        loss = jnp.where(here, highest + jnp.log(summed) - picked, 0.0)
        num_ref[0:1, :] = num_ref[0:1, :] + jnp.sum(loss)
        inverse = jnp.where(here, 1.0 / summed, 0.0)
        minus = jnp.where(here, 1.0, 0.0)
        dproj = 0.0
        for (low, high), part, hit in zip(groups, exped, targets):
            dscore = (part * inverse - jnp.where(hit, minus, 0.0)).astype(BF16)
            dproj = dproj + jnp.dot(dscore, acc_ref[low:high, :], preferred_element_type=F32)
        dproj = (dproj * scale).astype(BF16)
        grad_ref[...] += lax.dot_general(
            donors, dproj, (((0,), (0,)), ((), ())), preferred_element_type=F32
        )
        return carry

    lax.fori_loop(0, (count + MB - 1) // MB, block, 0)

    lanes = lax.broadcasted_iota(I32, (8, SUB), 1)
    sums_ref[...] = jnp.where(lanes == 0, num_ref[0:1, :], count.astype(F32))
    part = width // 8
    for m in range(4):
        keep = pl.multiple_of((2 * (x ^ m) + c) * part, 8)
        send = pl.multiple_of((2 * (x ^ m) + 1 - c) * part, 8)
        keep_ref[m] = grad_ref[pl.ds(keep, part), :]
        send_ref[m] = grad_ref[pl.ds(send, part), :].astype(BF16)


def combine_kernel(keep_ref, received_ref, sums_ref, other_ref, *out_refs):
    for m in range(4):
        out_refs[m][...] = (keep_ref[m] + received_ref[m].astype(F32)).astype(BF16)
    out_refs[4][...] = sums_ref[...] + other_ref[...]


def spread_kernel(own_ref, one_ref, two_ref, three_ref, out_ref):
    sums = (own_ref[...] + one_ref[...]) + (two_ref[...] + three_ref[...])
    out_ref[...] = jnp.broadcast_to(sums[None], out_ref.shape)


def local(
    donor_emb,
    acceptor_emb,
    donor_pos,
    acceptor_pos,
    donor_count,
    acceptor_count,
    target,
    junction_mask,
    weights,
):
    width = weights.shape[1]
    part = width // 8
    vmem = pl.BlockSpec(memory_space=pltpu.VMEM)
    smem = pl.BlockSpec(memory_space=pltpu.SMEM)
    any_space = pl.BlockSpec(memory_space=pl.ANY)
    sites = 2 * CAP
    block = pl.pallas_call(
        site_kernel,
        out_shape=jax.ShapeDtypeStruct((sites + 8, width), BF16),
        in_specs=[smem] * 3 + [any_space] * 4,
        out_specs=vmem,
        scratch_shapes=[
            pltpu.VMEM((8 * sites, width), BF16),
            pltpu.VMEM((2, 8, PIECE), I32),
            pltpu.SemaphoreType.DMA((sites + 2,)),
        ],
        name="site_rows",
    )(acceptor_pos, donor_pos, donor_count, acceptor_emb, donor_emb, target, junction_mask)
    lines = block[sites:]

    block = jnp.stack([block] + [exchange(block, "y", "z", m) for m in (1, 2, 3)])
    block = jnp.stack([block] + [exchange(block, "z", "x", m) for m in (1, 2, 3)])
    acceptors = jnp.concatenate([block[:, :, :CAP].reshape(PIECE, width), lines])
    donors = block[:, :, CAP:sites].reshape(PIECE, width)
    all_lines = block[:, 0, sites:]
    acceptors = [acceptors] + [exchange(acceptors, "x", "y", m) for m in (1, 2, 3)]
    donors = [donors] + [exchange(donors, "x", "y", m) for m in (1, 2, 3)]
    others = []
    for piece in acceptors:
        others.append(swap_core(piece))

    near = pltpu.MemorySpace.VMEM

    def call(kernel, limit, outs, operands, scratch=(), scalars=(), specs=vmem):
        operands = [pltpu.with_memory_space_constraint(o, near) for o in operands]
        return pl.pallas_call(
            kernel,
            out_shape=outs,
            in_specs=[smem] * len(scalars) + [vmem] * len(operands),
            out_specs=specs,
            scratch_shapes=list(scratch),
            compiler_params=pltpu.CompilerParams(vmem_limit_bytes=limit * 2**20),
        )(*scalars, *operands)

    compacted, offsets, values, ranks, starts = call(
        acceptor_kernel,
        24,
        (
            near((ROWS_A, width), BF16),
            near((8, SUB), I32),
            near((16, SUB), I32),
            near((16, SUB), I32),
            jax.ShapeDtypeStruct((16,), I32),
        ),
        (acceptor_count.reshape(1, 128), all_lines, *acceptors, *others),
        specs=(vmem,) * 4 + (smem,),
    )
    tissue = lax.dynamic_index_in_dim(weights, lax.axis_index("x"), 0, False)
    keep, send, sums = call(
        head_kernel,
        36,
        (
            near((4, part, width), F32),
            near((4, part, width), BF16),
            near((8, SUB), F32),
        ),
        (compacted, offsets, values, ranks, tissue, *donors),
        (
            pltpu.VMEM((4 * PIECE + MB + 16, width), BF16),
            pltpu.VMEM((4 * PIECE + MB + 16, SUB), I32),
            pltpu.VMEM((width, width), F32),
            pltpu.VMEM((8, SUB), F32),
        ),
        (starts,),
        specs=(vmem,) * 3,
    )

    other = swap_core(sums)
    received = swap_core(send)
    *total, sums = call(
        combine_kernel,
        12,
        (near((part, width), BF16),) * 4 + (near((8, SUB), F32),),
        (keep, received, sums, other),
        specs=(vmem,) * 5,
    )
    spread = [total[0]] + [exchange(total[m], "x", "x", m) for m in (1, 2, 3)]
    sums = call(
        spread_kernel,
        12,
        near((16, 8, SUB), F32),
        [sums] + [exchange(sums, "x", "x", m) for m in (1, 2, 3)],
    )
    sums = lax.all_to_all(sums, ("y", "z"), 0, 0, tiled=True)
    sums = jnp.sum(sums[:, 0, :2], axis=0)
    loss = sums[0] / jnp.maximum(sums[1], 1.0)

    grad_weight = call(output_kernel, 12, jax.ShapeDtypeStruct((part, 4, width), F32), spread)
    return (loss, grad_weight)


def solution(mesh):
    finer = Mesh(mesh.devices.reshape(SIZES), AXES)
    don, acc = ("x", "c"), ("y", "z")
    return jax.shard_map(
        local,
        mesh=finer,
        in_specs=(
            P(AXES, None),
            P(AXES, None),
            P(AXES),
            P(AXES),
            P(don),
            P(),
            P(None, don),
            P(None, don),
            P(acc, None, None),
        ),
        out_specs=(P(), P(don, acc, None)),
        check_vma=False,
    )
```

```python
import itertools

import jax
import jax.numpy as jnp
from jax import lax
from jax.experimental import pallas as pl
from jax.experimental.pallas import tpu as pltpu
from jax.sharding import Mesh
from jax.sharding import PartitionSpec as P


AXES = ("x", "c", "y", "z")
SIZES = (4, 2, 4, 4)
CAP = 24
LIVE = 1600
COLS = 1664
ROWS_A = 1744
MAIN = 1536
MB = 256
PIECE = 16 * CAP
SUB = 128
F32 = jnp.float32
BF16 = jnp.bfloat16
I32 = jnp.int32


def exchange_pairs(axis_core0, axis_core1, mask):
    pairs = []
    for coords in itertools.product(*(range(n) for n in SIZES)):
        moved = list(coords)
        axis = AXES.index(axis_core1 if coords[1] else axis_core0)
        moved[axis] ^= mask
        source = target = 0
        for n, a, b in zip(SIZES, coords, moved):
            source, target = source * n + a, target * n + b
        pairs.append((source, target))
    return pairs


def exchange(value, axis_core0, axis_core1, mask):
    return lax.ppermute(value, AXES, exchange_pairs(axis_core0, axis_core1, mask))


def swap_core(value):
    return lax.ppermute(value, "c", [(0, 1), (1, 0)])


def site_kernel(
    apos_ref,
    dpos_ref,
    count_ref,
    aemb_ref,
    demb_ref,
    target_ref,
    mask_ref,
    out_ref,
    line_ref,
    rows_ref,
    picked_ref,
    sems,
):
    sites = 2 * CAP
    copies = []
    picks = lax.broadcasted_iota(I32, (sites, 1), 0)
    lanes = lax.broadcasted_iota(I32, (sites, 8 * sites), 1)
    column = lax.axis_index("y") * 4 + lax.axis_index("z")
    tissues = pl.multiple_of((column // 2) * 8, 8)
    for i, ref in enumerate((target_ref, mask_ref)):
        copies.append(
            pltpu.make_async_copy(
                ref.at[pl.ds(tissues, 8), :], picked_ref.at[i], sems.at[sites + i]
            )
        )
        copies[-1].start()
    wanted = picks * 8
    for i in range(sites):
        emb_ref, pos = (aemb_ref, apos_ref[i]) if i < CAP else (demb_ref, dpos_ref[i - CAP])
        group = pl.multiple_of((pos // 8) * 8, 8)
        copies.append(
            pltpu.make_async_copy(
                emb_ref.at[pl.ds(group, 8), :], rows_ref.at[pl.ds(8 * i, 8), :], sems.at[i]
            )
        )
        copies[-1].start()
        wanted = jnp.where(picks == i, wanted + (pos - group), wanted)
    onehot = jnp.where(lanes == wanted, 1.0, 0.0).astype(BF16)

    lane = lax.broadcasted_iota(I32, (4, PIECE), 1)
    shard = (lane * 2731) >> 16
    limit = jnp.zeros((4, PIECE), I32)
    for i in range(16):
        limit = jnp.where(shard == i, count_ref[i], limit)
    live = lane - shard * CAP < limit
    for copy in copies[:2]:
        copy.wait()
    upper = column % 2 == 1
    targets = jnp.where(upper, picked_ref[0, 4:8, :], picked_ref[0, 0:4, :])
    masks = jnp.where(upper, picked_ref[1, 4:8, :], picked_ref[1, 0:4, :])
    value = jnp.where(live & (masks > 0), targets, -1)
    halves = jnp.concatenate([value >> 6, value & 63], axis=1).astype(F32)
    halves = jnp.concatenate([halves, jnp.zeros_like(halves)], axis=0)
    line_ref[...] = halves.astype(BF16)

    for copy in copies[2:]:
        copy.wait()
    out_ref[...] = jnp.dot(onehot, rows_ref[...], preferred_element_type=F32).astype(BF16)


def output_kernel(own_ref, one_ref, two_ref, three_ref, out_ref):
    x = lax.axis_index("x")
    for m, ref in enumerate((own_ref, one_ref, two_ref, three_ref)):
        out_ref[:, pl.ds(x ^ m, 1), :] = ref[...].astype(F32)[:, None, :]


def one_hot(hit):
    return jnp.where(hit, 1.0, 0.0).astype(BF16)


def as_rows(row):
    return jnp.broadcast_to(row, (8, SUB)).astype(BF16)


def acceptor_tables(count_row, x, c, y, z):
    lane = lax.broadcasted_iota(I32, (1, SUB), 1)
    sub = lax.broadcasted_iota(I32, (SUB, SUB), 0)
    part = lane >> 4
    m2, m1 = (lane >> 2) & 3, lane & 3
    half = jnp.where(part < 6, (part * 11) >> 5, part - 6)
    m3 = part - 3 * half
    m3 = jnp.where(part < 6, m3 ^ (m3 >> 1), 2)
    core = c ^ half
    shard0 = (x ^ m3) * 32 + (y ^ m1) * 4 + (z ^ m2)
    shard1 = (x ^ m2) * 32 + 16 + (y ^ m3) * 4 + (z ^ m1)
    shard = jnp.where(core == 0, shard0, shard1)
    counts = jnp.dot(
        as_rows(count_row.astype(F32)), one_hot(sub == shard), preferred_element_type=F32
    )
    offsets = jnp.dot(
        counts.astype(BF16), one_hot(sub < lane), preferred_element_type=F32
    ).astype(I32)
    counts_row = counts.astype(I32)[0:1, :]
    row = lax.broadcasted_iota(I32, (8, SUB), 0)
    table = jnp.where(row == 0, counts.astype(I32), jnp.where(row == 1, offsets >> 6, offsets & 63))
    table = table.astype(F32).astype(BF16)
    ranks, starts = [], []
    for b in range(8 * PIECE // SUB):
        slot = b * SUB + lane
        place = (slot * 2731) >> 16
        within = slot - place * CAP
        here = jnp.dot(table, one_hot(sub == place), preferred_element_type=F32).astype(I32)
        rank = here[1:2, :] * 64 + here[2:3, :] + within
        ranks.append(jnp.where(within < here[0:1, :], rank, -1))
        before = jnp.minimum(jnp.maximum(b * SUB - CAP * lane, 0), counts_row)
        starts.append(jnp.sum(before.astype(F32)).astype(I32))
    return offsets[0:1, :], ranks, starts


def donor_tables(rows, x, c, y, z):
    lane = lax.broadcasted_iota(I32, (1, SUB), 1)
    sub = lax.broadcasted_iota(I32, (SUB, SUB), 0)
    row = lax.broadcasted_iota(I32, (8, SUB), 0)
    pick = lax.broadcasted_iota(I32, (8, 2 * PIECE), 0) == x
    lines = [
        jnp.sum(jnp.where(pick, r.astype(F32), 0.0), axis=0, keepdims=True) for r in rows
    ]
    sources = []
    for u in range(PIECE // SUB):
        low, high = u * SUB, (u + 1) * SUB
        stack = [line[:, low:high] for line in lines]
        stack += [line[:, PIECE + low : PIECE + high] for line in lines]
        sources.append(jnp.concatenate(stack, axis=0).astype(BF16))
    values = []
    for m3 in range(4):
        for v in range(PIECE // SUB):
            slot = v * SUB + lane
            place = (slot * 2731) >> 16
            within = slot - place * CAP
            m2, m1 = place >> 2, place & 3
            natural0 = (y ^ m1) * 4 + (z ^ m2)
            natural1 = (y ^ m3) * 4 + (z ^ m1)
            natural = jnp.where(c == 0, natural0, natural1) * CAP + within
            wanted = jnp.where(c == 0, m3, m2)
            moved = sum(
                jnp.dot(source, one_hot(sub + u * SUB == natural), preferred_element_type=F32)
                for u, source in enumerate(sources)
            )
            moved = jnp.where((row & 3) == wanted, moved, 0.0)
            moved = moved * jnp.where(row < 4, 64.0, 1.0)
            values.append(jnp.sum(moved, axis=0, keepdims=True).astype(I32))
    return values


def compact(dst_ref, source, rank_row, start):
    base = pl.multiple_of((start // 16) * 16, 16)
    hit = lax.broadcasted_iota(I32, (SUB + 16, SUB), 0) == rank_row - base
    picked = jnp.dot(
        jnp.where(hit, 1.0, 0.0).astype(BF16), source, preferred_element_type=F32
    ).astype(BF16)
    dst_ref[pl.ds(base, 16), :] = dst_ref[pl.ds(base, 16), :] + picked[:16]
    dst_ref[pl.ds(base + 16, SUB), :] = picked[16:]
    return hit, base


def table_kernel(count_ref, one_ref, two_ref, three_ref, four_ref, weights_ref, *refs):
    offset_ref, arank_ref, value_ref, drank_ref, w_ref, astarts_ref, dstarts_ref, sem = refs
    x, c, y, z = (lax.axis_index(a) for a in AXES)
    copy = pltpu.make_async_copy(weights_ref.at[x], w_ref, sem)
    copy.start()
    lower = lax.broadcasted_iota(I32, (SUB, SUB), 0) <= lax.broadcasted_iota(I32, (SUB, SUB), 1)
    lower = one_hot(lower)
    rows = [ref[...] for ref in (one_ref, two_ref, three_ref, four_ref)]
    count = 0
    values = donor_tables(rows, x, c, y, z)
    for b, row in enumerate(values):
        dstarts_ref[b] = count
        active = jnp.where(row >= 0, 1.0, 0.0)
        inclusive = jnp.dot(as_rows(active), lower, preferred_element_type=F32).astype(I32)
        drank_ref[b : b + 1, :] = jnp.where(row >= 0, inclusive[0:1, :] - 1 + count, -1)
        value_ref[b : b + 1, :] = row
        count = count + jnp.sum(active).astype(I32)
    dstarts_ref[len(values)] = count
    offset_row, ranks, starts = acceptor_tables(count_ref[...], x, c, y, z)
    offset_ref[...] = jnp.broadcast_to(offset_row, (8, SUB))
    for b, (rank, start) in enumerate(zip(ranks, starts)):
        arank_ref[b : b + 1, :] = rank
        astarts_ref[b] = start
    copy.wait()


def acceptor_kernel(first, starts_ref, rank_ref, *refs):
    pieces, acc_ref = refs[:-1], refs[-1]
    width = acc_ref.shape[1]
    blocks = PIECE // SUB
    if first == 0:
        acc_ref[0:16, :] = jnp.zeros((16, width), BF16)
    else:
        pieces = pieces[1:]
    for i, piece in enumerate(pieces):
        for j in range(blocks):
            b = (first + i) * blocks + j
            source = piece[j * SUB : (j + 1) * SUB, :]
            compact(acc_ref, source, rank_ref[b : b + 1, :], starts_ref[b])
    if first:
        acc_ref[LIVE:COLS, :] = jnp.zeros((COLS - LIVE, width), BF16)


def head_kernel(starts_ref, acc_ref, offset_ref, value_ref, rank_ref, w_ref, *refs):
    pieces = refs[:4]
    keep_ref, send_ref, sums_ref = refs[4:7]
    rows_ref, tval_ref, grad_ref, num_ref = refs[7:]
    width = w_ref.shape[0]
    scale = width ** (-0.5)
    x, c, y, z = (lax.axis_index(a) for a in AXES)
    blocks = PIECE // SUB
    count = starts_ref[4 * blocks]
    offset_row = offset_ref[0:1, :]

    rows_ref[0:16, :] = jnp.zeros((16, width), BF16)
    tval_ref[0:16, :] = jnp.zeros((16, SUB), I32)
    grad_ref[...] = jnp.zeros((width, width), F32)
    num_ref[...] = jnp.zeros((8, SUB), F32)
    for b in range(4 * blocks):
        i, j = b // blocks, b % blocks
        source = pieces[i][j * SUB : (j + 1) * SUB, :]
        hit, base = compact(rows_ref, source, rank_ref[b : b + 1, :], starts_ref[b])
        chosen = jnp.sum(jnp.where(hit, value_ref[b : b + 1, :], 0), axis=1, keepdims=True)
        chosen = jnp.broadcast_to(chosen, (SUB + 16, SUB))
        tval_ref[pl.ds(base, 16), :] = tval_ref[pl.ds(base, 16), :] + chosen[:16]
        tval_ref[pl.ds(base + 16, SUB), :] = chosen[16:]
    tail = pl.multiple_of(((count + 15) // 16) * 16, 16)
    rows_ref[pl.ds(tail, MB), :] = jnp.zeros((MB, width), BF16)
    tval_ref[pl.ds(tail, MB), :] = jnp.zeros((MB, SUB), I32)

    def block(i, carry):
        first = pl.multiple_of(i * MB, MB)
        donors = rows_ref[pl.ds(first, MB), :]
        slot = tval_ref[pl.ds(first, MB), :]
        shard = (slot * 2731) >> 16
        within = slot - shard * CAP
        mx = (shard >> 5) ^ x
        core = (shard >> 4) & 1
        my = ((shard >> 2) & 3) ^ y
        mz = (shard & 3) ^ z
        half = jnp.where(core == c, 0, 1)
        m3 = jnp.where(core == 0, mx, my)
        part = jnp.where(m3 == 2, 6 + half, half * 3 + m3 - (m3 >> 1))
        place = part * 16 + jnp.where(core == 0, mz * 4 + my, mx * 4 + mz)
        found = place == lax.broadcasted_iota(I32, (MB, SUB), 1)
        column = jnp.sum(jnp.where(found, offset_row + within, 0), axis=1, keepdims=True)

        projected = jnp.dot(donors, w_ref[...], preferred_element_type=F32).astype(BF16)
        groups = ((0, MAIN), (MAIN, COLS))
        scores, targets = [], []
        for low, high in groups:
            part = lax.dot_general(
                projected,
                acc_ref[low:high, :],
                (((1,), (1,)), ((), ())),
                preferred_element_type=F32,
            )
            columns = low + lax.broadcasted_iota(I32, (MB, high - low), 1)
            part = part * scale
            if high > LIVE:
                part = jnp.where(columns < LIVE, part, -1e30)
            scores.append(part)
            targets.append(columns == column)
        highest = jnp.maximum(*(jnp.max(part, axis=1, keepdims=True) for part in scores))
        exped = [jnp.exp(part - highest) for part in scores]
        exped[1] = jnp.where(scores[1] > -1e29, exped[1], 0.0)
        summed = sum(jnp.sum(part, axis=1, keepdims=True) for part in exped)
        picked = sum(
            jnp.sum(jnp.where(hit, part, 0.0), axis=1, keepdims=True)
            for hit, part in zip(targets, scores)
        )
        here = first + lax.broadcasted_iota(I32, (MB, 1), 0) < count
        loss = jnp.where(here, highest + jnp.log(summed) - picked, 0.0)
        num_ref[0:1, :] = num_ref[0:1, :] + jnp.sum(loss)
        inverse = jnp.where(here, 1.0 / summed, 0.0)
        minus = jnp.where(here, 1.0, 0.0)
        dproj = 0.0
        for (low, high), part, hit in zip(groups, exped, targets):
            dscore = (part * inverse - jnp.where(hit, minus, 0.0)).astype(BF16)
            dproj = dproj + jnp.dot(dscore, acc_ref[low:high, :], preferred_element_type=F32)
        dproj = (dproj * scale).astype(BF16)
        grad_ref[...] += lax.dot_general(
            donors, dproj, (((0,), (0,)), ((), ())), preferred_element_type=F32
        )
        return carry

    lax.fori_loop(0, (count + MB - 1) // MB, block, 0)

    lanes = lax.broadcasted_iota(I32, (8, SUB), 1)
    sums_ref[...] = jnp.where(lanes == 0, num_ref[0:1, :], count.astype(F32))
    part = width // 8
    for m in range(4):
        keep = pl.multiple_of((2 * (x ^ m) + c) * part, 8)
        send = pl.multiple_of((2 * (x ^ m) + 1 - c) * part, 8)
        keep_ref[m] = grad_ref[pl.ds(keep, part), :]
        send_ref[m] = grad_ref[pl.ds(send, part), :].astype(BF16)


def combine_kernel(keep_ref, received_ref, sums_ref, other_ref, *out_refs):
    for m in range(4):
        out_refs[m][...] = (keep_ref[m] + received_ref[m].astype(F32)).astype(BF16)
    out_refs[4][...] = sums_ref[...] + other_ref[...]


def spread_kernel(own_ref, one_ref, two_ref, three_ref, out_ref):
    sums = (own_ref[...] + one_ref[...]) + (two_ref[...] + three_ref[...])
    out_ref[...] = jnp.broadcast_to(sums[None], out_ref.shape)


def local(
    donor_emb,
    acceptor_emb,
    donor_pos,
    acceptor_pos,
    donor_count,
    acceptor_count,
    target,
    junction_mask,
    weights,
):
    width = weights.shape[1]
    part = width // 8
    vmem = pl.BlockSpec(memory_space=pltpu.VMEM)
    smem = pl.BlockSpec(memory_space=pltpu.SMEM)
    any_space = pl.BlockSpec(memory_space=pltpu.MemorySpace.HBM)
    sites = 2 * CAP
    near = pltpu.MemorySpace.VMEM
    block, lines = pl.pallas_call(
        site_kernel,
        out_shape=(near((sites, width), BF16), near((8, width), BF16)),
        in_specs=[smem] * 3 + [any_space] * 4,
        out_specs=(vmem, vmem),
        scratch_shapes=[
            pltpu.VMEM((8 * sites, width), BF16),
            pltpu.VMEM((2, 8, PIECE), I32),
            pltpu.SemaphoreType.DMA((sites + 2,)),
        ],
        name="site_rows",
    )(acceptor_pos, donor_pos, donor_count, acceptor_emb, donor_emb, target, junction_mask)

    block = jnp.stack([block] + [exchange(block, "y", "z", m) for m in (1, 2, 3)])
    lines = [lines] + [exchange(lines, "x", "x", m) for m in (1, 2, 3)]
    block = jnp.stack([block] + [exchange(block, "z", "x", m) for m in (1, 2, 3)])
    acceptors = block[:, :, :CAP].reshape(PIECE, width)
    donors = block[:, :, CAP:sites].reshape(PIECE, width)
    acceptors = [acceptors] + [exchange(acceptors, "x", "y", m) for m in (1, 2, 3)]
    donors = [donors] + [exchange(donors, "x", "y", m) for m in (1, 2, 3)]
    others = []
    for piece in acceptors:
        others.append(swap_core(piece))

    def call(kernel, limit, outs, operands, scratch=(), scalars=(), specs=vmem, **options):
        operands = [pltpu.with_memory_space_constraint(o, near) for o in operands]
        return pl.pallas_call(
            kernel,
            out_shape=outs,
            in_specs=[smem] * len(scalars) + [vmem] * len(operands),
            out_specs=specs,
            scratch_shapes=list(scratch),
            compiler_params=pltpu.CompilerParams(vmem_limit_bytes=limit * 2**20),
            **options,
        )(*scalars, *operands)

    offsets, aranks, values, dranks, tissue, astarts, dstarts = pl.pallas_call(
        table_kernel,
        out_shape=(
            near((8, SUB), I32),
            near((24, SUB), I32),
            near((16, SUB), I32),
            near((16, SUB), I32),
            near((width, width), BF16),
            jax.ShapeDtypeStruct((24,), I32),
            jax.ShapeDtypeStruct((16,), I32),
        ),
        in_specs=[vmem] * 5 + [any_space],
        out_specs=(vmem,) * 5 + (smem,) * 2,
        scratch_shapes=[pltpu.SemaphoreType.DMA(())],
        compiler_params=pltpu.CompilerParams(vmem_limit_bytes=12 * 2**20),
        name="tables",
    )(acceptor_count.reshape(1, 128), *lines, weights)

    acc_shape = near((ROWS_A, width), BF16)
    early = [side[m] for side in (acceptors, others) for m in (0, 1, 3)]
    compacted = call(
        lambda *refs: acceptor_kernel(0, *refs), 16, acc_shape, [aranks] + early, scalars=(astarts,)
    )
    compacted = call(
        lambda starts_ref, rank_ref, *refs: acceptor_kernel(6, starts_ref, rank_ref, *refs),
        16,
        acc_shape,
        [aranks, compacted, acceptors[2], others[2]],
        scalars=(astarts,),
        input_output_aliases={2: 0},
    )
    keep, send, sums = call(
        head_kernel,
        36,
        (
            near((4, part, width), F32),
            near((4, part, width), BF16),
            near((8, SUB), F32),
        ),
        (compacted, offsets, values, dranks, tissue, *donors),
        (
            pltpu.VMEM((4 * PIECE + MB + 16, width), BF16),
            pltpu.VMEM((4 * PIECE + MB + 16, SUB), I32),
            pltpu.VMEM((width, width), F32),
            pltpu.VMEM((8, SUB), F32),
        ),
        (dstarts,),
        specs=(vmem,) * 3,
    )

    other = swap_core(sums)
    received = swap_core(send)
    *total, sums = call(
        combine_kernel,
        12,
        (near((part, width), BF16),) * 4 + (near((8, SUB), F32),),
        (keep, received, sums, other),
        specs=(vmem,) * 5,
    )
    spread = [total[0]] + [exchange(total[m], "x", "x", m) for m in (1, 2, 3)]
    sums = call(
        spread_kernel,
        12,
        near((16, 8, SUB), F32),
        [sums] + [exchange(sums, "x", "x", m) for m in (1, 2, 3)],
    )
    sums = lax.all_to_all(sums, ("y", "z"), 0, 0, tiled=True)
    sums = jnp.sum(sums[:, 0, :2], axis=0)
    loss = sums[0] / jnp.maximum(sums[1], 1.0)

    grad_weight = call(output_kernel, 12, jax.ShapeDtypeStruct((part, 4, width), F32), spread)
    return (loss, grad_weight)


def solution(mesh):
    finer = Mesh(mesh.devices.reshape(SIZES), AXES)
    don, acc = ("x", "c"), ("y", "z")
    return jax.shard_map(
        local,
        mesh=finer,
        in_specs=(
            P(AXES, None),
            P(AXES, None),
            P(AXES),
            P(AXES),
            P(don),
            P(),
            P(None, don),
            P(None, don),
            P(acc, None, None),
        ),
        out_specs=(P(), P(don, acc, None)),
        check_vma=False,
    )
```
